128 devices in a mesh: row: 32 (over x, z, core), col: 4 (over y).
Axes of the slice: x: 4, y: 4, z: 4, core: 2. Of those that a mesh axis runs over, the one named last changes fastest.
Arguments:
- eigvecs: bfloat16 [49152, 4096], P('row', 'col'), may hold values from -41 to 41
- reflectors: bfloat16 [8, 49152, 128], P(None, 'row'), as said below
- factors: float32 [8, 128, 128], replicated, as said below
Outputs:
- vectors: bfloat16 [49152, 4096], P('row', 'col')
- deviation: float32 [4096], P('col')
The draws below stay inside these ranges and needn't reach their ends.
Inputs may be any that keep to these rules, and one draw needn't show every extreme that they name: `reflectors`: each panel's vectors are dense and linearly independent. factors[k] is the upper triangular compact WY factor of reflectors[k]: its inverse plus its inverse's transpose equals reflectors[k]^T reflectors[k], so that I - reflectors[k] factors[k] reflectors[k]^T is orthogonal up to rounding.
All inputs are finite; a program needn't handle non-finite values.
Results may differ from the reference program's by a relative error of at most 0.014.
Values may be sent and summed in bfloat16 or wider, within the bound.
No kernel may reach another device: no remote copies, remote signals or barrier semaphores. Data moves between devices by JAX's collectives and lax.ppermute only.
A program may use at most 64 MiB of HBM per device.

```python
import jax
import jax.numpy as jnp
from jax import lax

NORD = 49152
M = 4096
B = 128
PANELS = 8


def reflector_panels(key):
    base = jax.random.fold_in(key, 7)
    first = jax.random.fold_in(base, 1)
    second = jax.random.fold_in(base, 2)
    third = jax.random.fold_in(base, 3)
    rough = jnp.clip(jax.random.normal(first, (PANELS, NORD, B), jnp.float32), -6.0, 6.0)
    weight = 0.4
    shared = jnp.clip(jax.random.normal(second, (PANELS, NORD, 1), jnp.float32), -6.0, 6.0)
    mixing = weight * jnp.clip(jax.random.normal(third, (PANELS, 1, B), jnp.float32), -6.0, 6.0)
    panels = (rough + shared * mixing) * NORD ** (-0.5)
    return panels.astype(jnp.bfloat16)


def draw_reflectors(key, part):
    return reflector_panels(key)


def draw_factors(key, part):
    panels = reflector_panels(key).astype(jnp.float32)
    gram = jnp.einsum('knb,knc->kbc', panels, panels, precision=lax.Precision.HIGHEST)
    eye = jnp.eye(B, dtype=jnp.float32)
    inverse = jnp.triu(gram, 1) + 0.5 * gram * eye[None, :, :]

    def invert(upper):
        return jax.scipy.linalg.solve_triangular(upper, eye, lower=False)
    return jax.vmap(invert)(inverse).astype(jnp.float32)


def draw_eigvecs(key, part):
    first = jax.random.fold_in(key, 21)
    second = jax.random.fold_in(key, 22)
    third = jax.random.fold_in(key, 23)
    fourth = jax.random.fold_in(key, 24)
    rows = jnp.arange(NORD).astype(jnp.float32) / NORD
    phase = jax.random.uniform(fourth, (), jnp.float32, 0.0, 1.0)
    entries = jnp.clip(jax.random.normal(first, (NORD, M), jnp.float32), -6.0, 6.0)
    amplitude = 0.8
    smooth = jnp.exp(amplitude * jnp.sin(6.2831853 * (2.0 * rows + phase)))
    rough = jnp.exp(jax.random.uniform(second, (NORD,), jnp.float32, -0.6931472, 0.6931472))
    columns = jnp.exp(jax.random.uniform(third, (M,), jnp.float32, -0.6931472, 0.4054651))
    values = entries * (smooth * rough)[:, None] * columns[None, :]
    return values.astype(jnp.bfloat16)


def setup_inputs(seed: int = 0) -> dict:
    seeds = jax.random.split(jax.random.key(seed), 4)
    return {
        "eigvecs": draw_eigvecs(jax.random.fold_in(seeds[3], 71), 0),
        "reflectors": draw_reflectors(jax.random.fold_in(seeds[3], 71), 0),
        "factors": draw_factors(jax.random.fold_in(seeds[3], 71), 0),
    }


def reference(eigvecs, reflectors, factors):
    vectors = eigvecs
    for panel in range(PANELS):
        basis = reflectors[panel]
        proj = jnp.dot(basis.T.astype(jnp.float32), vectors.astype(jnp.float32), preferred_element_type=jnp.float32)
        scaled = jnp.dot(factors[panel], proj, precision=lax.Precision.HIGHEST).astype(jnp.bfloat16)
        update = jnp.dot(basis.astype(jnp.float32), scaled.astype(jnp.float32), preferred_element_type=jnp.float32)
        vectors = (vectors.astype(jnp.float32) - update).astype(jnp.bfloat16)
    wide = vectors.astype(jnp.float32)
    squares = lax.optimization_barrier(jnp.sum(wide * wide, axis=0))
    deviation = jnp.sqrt(squares / NORD) - 1.0
    return (vectors, deviation)
```

```python
import functools

import jax
import jax.numpy as jnp
from jax import lax
from jax.experimental import pallas as pl
from jax.experimental.pallas import tpu as pltpu
from jax.sharding import Mesh
from jax.sharding import PartitionSpec as P

NORD = 49152
WIDTH = 128
PANELS = 8
CHIPS = 16
OWN = 32
HALF = CHIPS * OWN
SHARE = 112
PAIRS = PANELS * (PANELS - 1) // 2
BF = jnp.bfloat16
F32 = jnp.float32
CHIP = ("x", "z")
ROW = ("x", "z", "core")
VMEM = pl.BlockSpec(memory_space=pltpu.VMEM)
SMEM = pl.BlockSpec(memory_space=pltpu.SMEM)


def call(kernel, out_shape, in_specs, out_specs, flops, nbytes, limit=24, **kw):
    return pl.pallas_call(
        kernel,
        out_shape=out_shape,
        in_specs=in_specs,
        out_specs=out_specs,
        compiler_params=pltpu.CompilerParams(vmem_limit_bytes=limit * 2**20),
        cost_estimate=pl.CostEstimate(flops=flops, bytes_accessed=nbytes, transcendentals=0),
        **kw,
    )


def first_block(k):
    return k * (k - 1) // 2


def gram_kernel(v_ref, g_ref):
    for j in range(0, PANELS - 1, 2):
        left = jnp.concatenate([v_ref[j], v_ref[j + 1]], axis=1)
        for k in range(j + 1, PANELS, 2):
            right = v_ref[k]
            if k + 1 < PANELS:
                right = jnp.concatenate([right, v_ref[k + 1]], axis=1)
            both = lax.dot_general(
                left, right, (((0,), (0,)), ((), ())), preferred_element_type=F32
            ).astype(BF)
            for dj in range(2):
                for dk in range(right.shape[1] // WIDTH):
                    jj, kk = j + dj, k + dk
                    if jj < kk:
                        at = (first_block(kk) + jj) * WIDTH
                        g_ref[at : at + WIDTH, :] = both[
                            dj * WIDTH : (dj + 1) * WIDTH, dk * WIDTH : (dk + 1) * WIDTH
                        ]


def proj_kernel(flip, core_ref, x_ref, v_ref, p_ref):
    half = core_ref[0]
    if flip:
        half = 1 - half
    step = 256
    for n in range(0, HALF, step):
        at = pl.multiple_of(half * HALF + n, step)
        x = x_ref[:, pl.ds(at, step)]
        xt = x.T
        for k in range(0, PANELS, 2):
            right = jnp.concatenate([v_ref[k], v_ref[k + 1]], axis=1)
            both = jnp.dot(xt, right, preferred_element_type=F32).astype(p_ref.dtype)
            first = n // OWN
            for dk in range(2):
                p_ref[first : first + step // OWN, (k + dk) * OWN : (k + dk + 1) * OWN, :] = both[
                    :, dk * WIDTH : (dk + 1) * WIDTH
                ].reshape(step // OWN, OWN, WIDTH)


def combine_kernel(own_ref, other_ref, g_ref, out_ref):
    share = g_ref[0].astype(F32)
    for r in range(1, 2 * CHIPS):
        share = share + g_ref[r].astype(F32)
    share = share.astype(BF)
    for s in range(CHIPS):
        out_ref[s, : PANELS * OWN, :] = (own_ref[s] + other_ref[s].astype(F32)).astype(BF)
        out_ref[s, PANELS * OWN :, :] = share


def solve_kernel(core_ref, mine_ref, theirs_ref, t_ref, out_ref, g_ref):
    core = core_ref[0]
    for s in range(CHIPS):
        at = pl.multiple_of((2 * s + core) * SHARE, 16)
        g_ref[pl.ds(at, SHARE), :] = mine_ref[s, PANELS * OWN :, :]
        at = pl.multiple_of((2 * s + 1 - core) * SHARE, 16)
        g_ref[pl.ds(at, SHARE), :] = theirs_ref[s]
    done = []
    for k in range(PANELS):
        rows = slice(k * OWN, (k + 1) * OWN)
        proj = mine_ref[0, rows, :].astype(F32)
        for s in range(1, CHIPS):
            proj = proj + mine_ref[s, rows, :].astype(F32)
        if k:
            at = first_block(k) * WIDTH
            cross = g_ref[at : at + k * WIDTH, :]
            before = jnp.concatenate(done, axis=1) if k > 1 else done[0]
            proj = proj - jnp.dot(before, cross, preferred_element_type=F32)
        scaled = lax.dot_general(
            proj,
            t_ref[k],
            (((1,), (1,)), ((), ())),
            precision=lax.Precision.HIGHEST,
            preferred_element_type=F32,
        ).astype(BF)
        done.append(scaled)
        for s in range(CHIPS):
            out_ref[s, rows, :] = scaled


def update_kernel(half_ref, x_ref, v_ref, s_ref, *refs):
    out_ref, sq_ref = refs[-2:]
    left = jnp.concatenate([v_ref[k] for k in range(PANELS)], axis=1)
    right = jnp.concatenate(
        [s_ref[:, k * OWN : (k + 1) * OWN, :].reshape(HALF, WIDTH) for k in range(PANELS)], axis=1
    )
    update = lax.dot_general(left, right, (((1,), (1,)), ((), ())), preferred_element_type=F32)
    out = (x_ref[...].astype(F32) - update).astype(BF)
    out_ref[...] = out
    wide = out.astype(F32)
    squares = jnp.sum(wide * wide, axis=0, keepdims=True)

    @pl.when(pl.program_id(0) == 0)
    def _():
        sq_ref[...] = squares

    @pl.when(pl.program_id(0) > 0)
    def _():
        sq_ref[...] += squares


def update(half, eigvecs, reflectors, scaled, so_far=None):
    rows, columns = eigvecs.shape
    block = 256
    in_specs = [
        pl.BlockSpec((block, HALF), lambda i, h: (i, h[0])),
        pl.BlockSpec((PANELS, block, WIDTH), lambda i, h: (0, i, 0)),
        pl.BlockSpec((CHIPS, PANELS * OWN, WIDTH), lambda i, h: (0, 0, 0)),
    ]
    args = [half, eigvecs, reflectors, scaled]
    aliases = {}
    if so_far is not None:
        in_specs.append(pl.BlockSpec(memory_space=pl.ANY))
        args.append(so_far)
        aliases = {4: 0}
    return pl.pallas_call(
        update_kernel,
        out_shape=(
            jax.ShapeDtypeStruct((rows, columns), BF),
            jax.ShapeDtypeStruct((1, HALF), F32),
        ),
        grid_spec=pltpu.PrefetchScalarGridSpec(
            num_scalar_prefetch=1,
            grid=(rows // block,),
            in_specs=in_specs,
            out_specs=(
                pl.BlockSpec((block, HALF), lambda i, h: (i, h[0])),
                pl.BlockSpec((1, HALF), lambda i, h: (0, 0)),
            ),
        ),
        input_output_aliases=aliases,
        compiler_params=pltpu.CompilerParams(
            vmem_limit_bytes=24 * 2**20, dimension_semantics=("arbitrary",)
        ),
        cost_estimate=pl.CostEstimate(
            flops=2 * rows * HALF * PANELS * WIDTH, bytes_accessed=6 * 2**20, transcendentals=0
        ),
    )(*args)


def swapped(value):
    return lax.ppermute(value, "core", [(0, 1), (1, 0)])


def exchanged(value, axes):
    return lax.all_to_all(value, axes, split_axis=0, concat_axis=0, tiled=True)


def body(eigvecs, reflectors, factors):
    rows = eigvecs.shape[0]
    core = lax.axis_index("core").astype(jnp.int32).reshape(1)
    flops = 2 * rows * HALF * PANELS * WIDTH
    gram = call(
        gram_kernel, jax.ShapeDtypeStruct((PAIRS * WIDTH, WIDTH), BF), [VMEM], VMEM, flops, 4 * 2**20
    )(reflectors)
    gram_parts = exchanged(gram.reshape(2 * CHIPS, SHARE, WIDTH), ROW)

    def proj(flip, dtype):
        return call(
            functools.partial(proj_kernel, flip),
            jax.ShapeDtypeStruct((CHIPS, PANELS * OWN, WIDTH), dtype),
            [SMEM, VMEM, VMEM],
            VMEM,
            flops,
            6 * 2**20,
        )(core, eigvecs, reflectors)

    other = swapped(proj(True, BF))
    own = proj(False, F32)
    payload = call(
        combine_kernel,
        jax.ShapeDtypeStruct((CHIPS, PANELS * OWN + SHARE, WIDTH), BF),
        [VMEM] * 3,
        VMEM,
        2**20,
        4 * 2**20,
    )(own, other, gram_parts)
    mine = exchanged(payload, CHIP)
    theirs = swapped(mine[:, PANELS * OWN :, :])
    scaled = call(
        solve_kernel,
        jax.ShapeDtypeStruct((CHIPS, PANELS * OWN, WIDTH), BF),
        [SMEM] + [VMEM] * 3,
        VMEM,
        2**26,
        4 * 2**20,
        scratch_shapes=[pltpu.VMEM((PAIRS * WIDTH, WIDTH), BF)],
    )(core, mine, theirs, factors)
    scaled_mine = exchanged(scaled, CHIP)
    scaled_theirs = swapped(scaled_mine)
    vectors, squares_mine = update(core, eigvecs, reflectors, scaled_mine)
    vectors, squares_theirs = update(1 - core, eigvecs, reflectors, scaled_theirs, vectors)
    both = jnp.concatenate([squares_mine, squares_theirs], axis=0)
    first = core[0] == 0
    local = jnp.where(first, both, both[::-1]).reshape(1, -1)
    everything = exchanged(jnp.broadcast_to(local, (2 * CHIPS, local.shape[1])), ROW)
    deviation = jnp.sqrt(jnp.sum(everything, axis=0) / NORD) - 1.0
    return (vectors, deviation)


def solution(mesh):
    split = Mesh(mesh.devices.reshape(4, 4, 2, 4), ("x", "z", "core", "col"))
    placed = (P(ROW, "col"), P(None, ROW, None), P())
    return jax.shard_map(
        body, mesh=split, in_specs=placed, out_specs=(P(ROW, "col"), P("col")), check_vma=False
    )
```

```python
import functools

import jax
import jax.numpy as jnp
from jax import lax
from jax.experimental import pallas as pl
from jax.experimental.pallas import tpu as pltpu
from jax.sharding import Mesh
from jax.sharding import PartitionSpec as P

NORD = 49152
WIDTH = 128
PANELS = 8
CHIPS = 16
OWN = 32
HALF = CHIPS * OWN
COLS = 4
SHARE = 32
PAIRS = PANELS * (PANELS - 1) // 2
FULL = 52
BF = jnp.bfloat16
F32 = jnp.float32
CHIP = ("x", "z")
ROW = ("x", "z", "core")
VMEM = pl.BlockSpec(memory_space=pltpu.VMEM)
SMEM = pl.BlockSpec(memory_space=pltpu.SMEM)
HBM = pl.BlockSpec(memory_space=pltpu.HBM)


def call(kernel, out_shape, in_specs, out_specs, flops, nbytes, limit=12, **kw):
    return pl.pallas_call(
        kernel,
        out_shape=out_shape,
        in_specs=in_specs,
        out_specs=out_specs,
        compiler_params=pltpu.CompilerParams(vmem_limit_bytes=limit * 2**20),
        cost_estimate=pl.CostEstimate(flops=flops, bytes_accessed=nbytes, transcendentals=0),
        **kw,
    )


def first_block(k):
    return k * (k - 1) // 2


def block_plan():
    twos, ones = [], []
    for j in range(PANELS - 1):
        ks = list(range(j + 1, PANELS))
        while len(ks) > 1:
            twos.append((j, ks.pop(0), ks.pop(0)))
        ones.extend((j, k, k) for k in ks)
    return [twos[3 * c : 3 * c + 3] + [ones[c]] for c in range(COLS)]


PLAN = block_plan()


def load(source, target, sem):
    copy = pltpu.make_async_copy(source, target, sem)
    copy.start()
    return copy


def gram_kernel(col_ref, v_hbm, g_ref, v_ref, sems):
    copies = [load(v_hbm.at[k], v_ref.at[k], sems.at[k]) for k in range(PANELS)]
    for copy in copies:
        copy.wait()
    col = col_ref[0]
    for i in range(COLS):
        index = [jnp.int32(PLAN[COLS - 1][i][n]) for n in range(3)]
        for c in range(COLS - 1):
            index = [jnp.where(col == c, PLAN[c][i][n], index[n]) for n in range(3)]
        j, k, l = index
        right = jnp.concatenate([v_ref[k], v_ref[l]], axis=1)
        both = jnp.dot(v_ref[j].T, right, preferred_element_type=F32).astype(BF)
        g_ref[2 * i * WIDTH : (2 * i + 1) * WIDTH, :] = both[:, :WIDTH]
        g_ref[(2 * i + 1) * WIDTH : (2 * i + 2) * WIDTH, :] = both[:, WIDTH:]


def share_kernel(g_ref, out_ref):
    share = g_ref[0].astype(F32)
    for r in range(1, 2 * CHIPS):
        share = share + g_ref[r].astype(F32)
    for c in range(COLS):
        out_ref[c] = share.astype(BF)


def proj_kernel(flip, core_ref, x_hbm, v_hbm, after_ref, p_ref, x_ref, v_ref, x_sems, v_sems):
    half = core_ref[0]
    if flip:
        half = 1 - half
    step = x_ref.shape[2]
    tiles = HALF // step

    def load_tile(n):
        at = pl.multiple_of(half * HALF + n * step, step)
        return load(x_hbm.at[:, pl.ds(at, step)], x_ref.at[n], x_sems.at[n])

    x_copies = [load_tile(0)]
    v_copies = [load(v_hbm.at[k], v_ref.at[k], v_sems.at[k]) for k in range(PANELS)]
    x_copies += [load_tile(n) for n in range(1, tiles)]
    for n in range(tiles):
        x_copies[n].wait()
        xt = x_ref[n].T
        for k in range(0, PANELS, 2):
            if n == 0:
                v_copies[k].wait()
                v_copies[k + 1].wait()
            right = jnp.concatenate([v_ref[k], v_ref[k + 1]], axis=1)
            both = jnp.dot(xt, right, preferred_element_type=F32).astype(p_ref.dtype)
            chips = slice(n * step // OWN, (n + 1) * step // OWN)
            for dk in range(2):
                p_ref[chips, (k + dk) * OWN : (k + dk + 1) * OWN, :] = both[
                    :, dk * WIDTH : (dk + 1) * WIDTH
                ].reshape(step // OWN, OWN, WIDTH)


def combine_kernel(own_ref, other_ref, g_ref, out_ref):
    for s in range(CHIPS):
        out_ref[s, : PANELS * OWN, :] = (own_ref[s].astype(F32) + other_ref[s].astype(F32)).astype(BF)
        for c in range(COLS):
            at = PANELS * OWN + c * SHARE
            out_ref[s, at : at + SHARE, :] = g_ref[c]


def solve_kernel(core_ref, mine_ref, theirs_ref, t_ref, out_ref, g_ref):
    core = core_ref[0]
    for c in range(COLS):
        for s in range(CHIPS):
            j, *ks = PLAN[c][s // 4]
            k = ks[s // 2 % 2]
            if s // 4 == 3 and s // 2 % 2:
                continue
            base = (first_block(k) + j) * WIDTH + s % 2 * 2 * SHARE
            rows = slice(c * SHARE, (c + 1) * SHARE)
            g_ref[pl.ds(pl.multiple_of(base + core * SHARE, SHARE), SHARE), :] = mine_ref[
                s, PANELS * OWN + c * SHARE : PANELS * OWN + (c + 1) * SHARE, :
            ]
            g_ref[pl.ds(pl.multiple_of(base + (1 - core) * SHARE, SHARE), SHARE), :] = theirs_ref[
                s, rows, :
            ]
    done = []
    for k in range(PANELS):
        rows = slice(k * OWN, (k + 1) * OWN)
        proj = mine_ref[0, rows, :].astype(F32)
        for s in range(1, CHIPS):
            proj = proj + mine_ref[s, rows, :].astype(F32)
        if k:
            at = first_block(k) * WIDTH
            cross = g_ref[at : at + k * WIDTH, :]
            before = jnp.concatenate(done, axis=1) if k > 1 else done[0]
            proj = proj - jnp.dot(before, cross, preferred_element_type=F32)
        scaled = lax.dot_general(
            proj,
            t_ref[k],
            (((1,), (1,)), ((), ())),
            precision=lax.Precision.HIGHEST,
            preferred_element_type=F32,
        ).astype(BF)
        done.append(scaled)
        for s in range(CHIPS):
            out_ref[s, rows, :] = scaled


def update_kernel(half_ref, x_hbm, v_hbm, s_ref, *refs):
    out_hbm, sq_ref, x_ref, v_ref, out_ref, sems, out_sems = refs[-7:]
    blocks = x_ref.shape[0]
    block = x_ref.shape[1]
    step = 256
    columns = pl.ds(pl.multiple_of(half_ref[0] * HALF, HALF), HALF)
    copies = []
    for i in range(blocks):
        rows = slice(i * block, (i + 1) * block)
        copies.append(
            [
                load(v_hbm.at[:, rows, :], v_ref.at[i], sems.at[2 * i]),
                load(x_hbm.at[rows, columns], x_ref.at[i], sems.at[2 * i + 1]),
            ]
        )
    squares = [jnp.zeros((1, step), F32)] * (HALF // step)
    stores = []
    for i in range(blocks):
        for copy in copies[i]:
            copy.wait()
        left = jnp.concatenate([v_ref[i, k] for k in range(PANELS)], axis=1)
        for n in range(0, HALF, step):
            chips = slice(n // OWN, (n + step) // OWN)
            right = jnp.concatenate(
                [
                    s_ref[chips, k * OWN : (k + 1) * OWN, :].reshape(step, WIDTH)
                    for k in range(PANELS)
                ],
                axis=1,
            )
            update = lax.dot_general(
                left, right, (((1,), (1,)), ((), ())), preferred_element_type=F32
            )
            out = (x_ref[i, :, n : n + step].astype(F32) - update).astype(BF)
            out_ref[i, :, n : n + step] = out
            wide = out.astype(F32)
            squares[n // step] += jnp.sum(wide * wide, axis=0, keepdims=True)
        rows = slice(i * block, (i + 1) * block)
        stores.append(load(out_ref.at[i], out_hbm.at[rows, columns], out_sems.at[i]))
    sq_ref[...] = jnp.concatenate(squares, axis=1)
    for store in stores:
        store.wait()


def update(half, eigvecs, reflectors, scaled, so_far=None):
    rows, columns = eigvecs.shape
    blocks = 3
    in_specs = [SMEM, HBM, HBM, VMEM]
    args = [half, eigvecs, reflectors, scaled]
    aliases = {}
    if so_far is not None:
        in_specs.append(HBM)
        args.append(so_far)
        aliases = {4: 0}
    return call(
        update_kernel,
        (
            jax.ShapeDtypeStruct((rows, columns), BF),
            jax.ShapeDtypeStruct((1, HALF), F32),
        ),
        in_specs,
        (HBM, VMEM),
        2 * rows * HALF * PANELS * WIDTH,
        6 * 2**20,
        limit=FULL,
        input_output_aliases=aliases,
        scratch_shapes=[
            pltpu.VMEM((blocks, rows // blocks, HALF), BF),
            pltpu.VMEM((blocks, PANELS, rows // blocks, WIDTH), BF),
            pltpu.VMEM((blocks, rows // blocks, HALF), BF),
            pltpu.SemaphoreType.DMA((2 * blocks,)),
            pltpu.SemaphoreType.DMA((blocks,)),
        ],
    )(*args)


def swapped(value):
    return lax.ppermute(value, "core", [(0, 1), (1, 0)])


def exchanged(value, axes):
    return lax.all_to_all(value, axes, split_axis=0, concat_axis=0, tiled=True)


def steps(eigvecs, reflectors, factors):
    rows = eigvecs.shape[0]
    core = lax.axis_index("core").astype(jnp.int32).reshape(1)
    flops = 2 * rows * HALF * PANELS * WIDTH
    col = lax.axis_index("col").astype(jnp.int32).reshape(1)
    gram = call(
        gram_kernel,
        jax.ShapeDtypeStruct((2 * COLS * WIDTH, WIDTH), BF),
        [SMEM, HBM],
        VMEM,
        flops // 2,
        4 * 2**20,
        limit=FULL,
        scratch_shapes=[
            pltpu.VMEM(reflectors.shape, BF),
            pltpu.SemaphoreType.DMA((PANELS,)),
        ],
    )(col, reflectors)
    gram_parts = exchanged(gram.reshape(2 * CHIPS, SHARE, WIDTH), ROW)
    share = call(
        share_kernel,
        jax.ShapeDtypeStruct((COLS, SHARE, WIDTH), BF),
        [VMEM],
        VMEM,
        2**18,
        2**18,
    )(gram_parts)
    shares = exchanged(share, "col")

    def proj(flip):
        step = 256
        return call(
            functools.partial(proj_kernel, flip),
            jax.ShapeDtypeStruct((CHIPS, PANELS * OWN, WIDTH), BF),
            [SMEM, HBM, HBM, HBM],
            VMEM,
            flops,
            6 * 2**20,
            limit=FULL,
            scratch_shapes=[
                pltpu.VMEM((HALF // step, rows, step), BF),
                pltpu.VMEM(reflectors.shape, BF),
                pltpu.SemaphoreType.DMA((HALF // step,)),
                pltpu.SemaphoreType.DMA((PANELS,)),
            ],
        )(core, eigvecs, reflectors, gram)

    other = proj(True)
    other = swapped(other)
    own = proj(False)
    payload = call(
        combine_kernel,
        jax.ShapeDtypeStruct((CHIPS, PANELS * OWN + COLS * SHARE, WIDTH), BF),
        [VMEM] * 3,
        VMEM,
        2**20,
        4 * 2**20,
    )(own, other, shares)
    mine = exchanged(payload, CHIP)
    theirs = swapped(mine[:, PANELS * OWN :, :])
    scaled = call(
        solve_kernel,
        jax.ShapeDtypeStruct((CHIPS, PANELS * OWN, WIDTH), BF),
        [SMEM] + [VMEM] * 3,
        VMEM,
        2**26,
        4 * 2**20,
        scratch_shapes=[pltpu.VMEM((PAIRS * WIDTH, WIDTH), BF)],
    )(core, mine, theirs, factors)
    scaled_mine = exchanged(scaled, CHIP)
    scaled_theirs = swapped(scaled_mine)
    vectors, squares_mine = update(core, eigvecs, reflectors, scaled_mine)
    vectors, squares_theirs = update(1 - core, eigvecs, reflectors, scaled_theirs, vectors)
    both = jnp.concatenate([squares_mine, squares_theirs], axis=0)
    first = core[0] == 0
    local = jnp.where(first, both, both[::-1]).reshape(1, -1)
    everything = exchanged(jnp.broadcast_to(local, (2 * CHIPS, local.shape[1])), ROW)
    deviation = jnp.sqrt(jnp.sum(everything, axis=0) / NORD) - 1.0
    return (vectors, deviation)


def solution(mesh):
    split = Mesh(mesh.devices.reshape(4, 4, 2, 4), ("x", "z", "core", "col"))
    placed = (P(ROW, "col"), P(None, ROW, None), P())
    return jax.shard_map(
        steps, mesh=split, in_specs=placed, out_specs=(P(ROW, "col"), P("col")), check_vma=False
    )
```

```python
import functools

import jax
import jax.numpy as jnp
from jax import lax
from jax.experimental import pallas as pl
from jax.experimental.pallas import tpu as pltpu
from jax.sharding import Mesh
from jax.sharding import PartitionSpec as P

NORD = 49152
WIDTH = 128
PANELS = 8
CHIPS = 16
OWN = 32
HALF = CHIPS * OWN
PAIRS = PANELS * (PANELS - 1) // 2
SHARE = PAIRS * WIDTH // (2 * CHIPS)
PROJ = PANELS * OWN
CHUNK = PROJ + SHARE
STEP = 256
BF = jnp.bfloat16
F32 = jnp.float32
CHIP = ("x", "z")
ROW = ("x", "z", "core")
VMEM = pl.BlockSpec(memory_space=pltpu.VMEM)
HBM = pl.BlockSpec(memory_space=pltpu.HBM)


def call(kernel, out_shape, in_specs, out_specs, flops, nbytes, limit=12, **kw):
    return pl.pallas_call(
        kernel,
        out_shape=out_shape,
        in_specs=in_specs,
        out_specs=out_specs,
        compiler_params=pltpu.CompilerParams(vmem_limit_bytes=limit * 2**20),
        cost_estimate=pl.CostEstimate(flops=flops, bytes_accessed=nbytes, transcendentals=0),
        **kw,
    )


def first_block(k):
    return k * (k - 1) // 2


def load(source, target, sem):
    copy = pltpu.make_async_copy(source, target, sem)
    copy.start()
    return copy


def pair(v_ref, k):
    return jnp.concatenate([v_ref[k], v_ref[k + 1]], axis=1)


def project(x_ref, v_ref, half, p_ref, ready=None):
    for n in range(0, HALF, STEP):
        if ready is not None:
            ready(n // STEP)
        at = pl.multiple_of(half * HALF + n, STEP)
        xt = x_ref[:, pl.ds(at, STEP)].T
        chips = slice(n // OWN, (n + STEP) // OWN)
        for k in range(0, PANELS, 2):
            both = jnp.dot(xt, pair(v_ref, k), preferred_element_type=F32).astype(BF)
            for dk in range(2):
                p_ref[chips, (k + dk) * OWN : (k + dk + 1) * OWN, :] = both[
                    :, dk * WIDTH : (dk + 1) * WIDTH
                ].reshape(STEP // OWN, OWN, WIDTH)


def first_kernel(x_hbm, v_hbm, other_ref, mine_ref, x_ref, v_ref, g_ref, x_sems, v_sems):
    core = lax.axis_index("core")
    v_copies = [load(v_hbm.at[k], v_ref.at[k], v_sems.at[k]) for k in range(PANELS)]
    x_copies = []
    for i, half in enumerate((1 - core, core)):
        for n in range(0, HALF, STEP):
            at = pl.ds(pl.multiple_of(half * HALF + n, STEP), STEP)
            x_copies.append(
                load(x_hbm.at[:, at], x_ref.at[:, at], x_sems.at[i * HALF // STEP + n // STEP])
            )
    for k in range(0, PANELS, 2):
        v_copies[k].wait()
        v_copies[k + 1].wait()
        right = pair(v_ref, k)
        for j in range(0, k + 1, 2):
            both = jnp.dot(pair(v_ref, j).T, right, preferred_element_type=F32).astype(BF)
            for dj in range(2):
                for dk in range(2):
                    if j + dj < k + dk:
                        at = (first_block(k + dk) + j + dj) * WIDTH
                        g_ref[at : at + WIDTH, :] = both[
                            dj * WIDTH : (dj + 1) * WIDTH, dk * WIDTH : (dk + 1) * WIDTH
                        ]
    for s in range(CHIPS):
        at = pl.multiple_of((1 - core) * CHIPS * SHARE + s * SHARE, 16)
        other_ref[s, PROJ:, :] = g_ref[pl.ds(at, SHARE), :]
        at = pl.multiple_of(core * CHIPS * SHARE + s * SHARE, 16)
        mine_ref[s] = g_ref[pl.ds(at, SHARE), :]
    project(x_ref, v_ref, 1 - core, other_ref, ready=lambda n: x_copies[n].wait())
    for copy in x_copies[HALF // STEP :]:
        copy.wait()


def own_kernel(x_ref, v_ref, p_ref):
    project(x_ref, v_ref, lax.axis_index("core"), p_ref)


def combine_kernel(own_ref, gram_ref, other_ref, out_ref):
    for s in range(CHIPS):
        out_ref[s, :PROJ, :] = (
            own_ref[s].astype(F32) + other_ref[s, :PROJ, :].astype(F32)
        ).astype(BF)
        out_ref[s, PROJ:, :] = (
            gram_ref[s].astype(F32) + other_ref[s, PROJ:, :].astype(F32)
        ).astype(BF)


def sum_kernel(parts_ref, out_ref):
    rows = 16
    for at in range(0, CHUNK, rows):
        total = parts_ref[0, at : at + rows, :].astype(F32)
        for s in range(1, CHIPS):
            total = total + parts_ref[s, at : at + rows, :].astype(F32)
        total = total.astype(BF)
        for s in range(CHIPS):
            out_ref[s, at : at + rows, :] = total


def split(value):
    high = value.astype(BF)
    return high, (value - high.astype(F32)).astype(BF)


def solve_kernel(mine_ref, theirs_ref, t_ref, out_ref, g_ref):
    core = lax.axis_index("core")
    for s in range(CHIPS):
        at = pl.multiple_of(core * CHIPS * SHARE + s * SHARE, 16)
        g_ref[pl.ds(at, SHARE), :] = mine_ref[s, PROJ:, :]
        at = pl.multiple_of((1 - core) * CHIPS * SHARE + s * SHARE, 16)
        g_ref[pl.ds(at, SHARE), :] = theirs_ref[s]
    groups = range(0, CHIPS, CHIPS // 2)
    done = [[] for _ in groups]
    for k in range(PANELS):
        rows = slice(k * OWN, (k + 1) * OWN)
        factor, rest = split(t_ref[k])
        factor = jnp.concatenate([factor, factor, rest], axis=1)
        for i, g in enumerate(groups):
            chips = slice(g, g + CHIPS // 2)
            proj = mine_ref[chips, rows, :].reshape(HALF // 2, WIDTH).astype(F32)
            if k:
                at = first_block(k) * WIDTH
                cross = g_ref[at : at + k * WIDTH, :]
                before = jnp.concatenate(done[i], axis=1) if k > 1 else done[i][0]
                proj = proj - jnp.dot(before, cross, preferred_element_type=F32)
            high, low = split(proj)
            scaled = lax.dot_general(
                jnp.concatenate([high, low, high], axis=1),
                factor,
                (((1,), (1,)), ((), ())),
                preferred_element_type=F32,
            ).astype(BF)
            done[i].append(scaled)
            out_ref[chips, rows, :] = scaled.reshape(CHIPS // 2, OWN, WIDTH)


def update_kernel(flip, x_ref, v_ref, s_ref, *refs):
    out_hbm, sq_ref, out_ref, sems = refs[-4:]
    half = lax.axis_index("core")
    if flip:
        half = 1 - half
    blocks, block = out_ref.shape[:2]
    columns = pl.ds(pl.multiple_of(half * HALF, HALF), HALF)
    squares = [jnp.zeros((1, STEP), F32)] * (HALF // STEP)
    stores = []
    for i in range(blocks):
        rows = slice(i * block, (i + 1) * block)
        left = jnp.concatenate([v_ref[k, rows, :] for k in range(PANELS)], axis=1)
        for n in range(0, HALF, STEP):
            chips = slice(n // OWN, (n + STEP) // OWN)
            right = jnp.concatenate(
                [
                    s_ref[chips, k * OWN : (k + 1) * OWN, :].reshape(STEP, WIDTH)
                    for k in range(PANELS)
                ],
                axis=1,
            )
            update = lax.dot_general(
                left, right, (((1,), (1,)), ((), ())), preferred_element_type=F32
            )
            x = x_ref[rows, pl.ds(pl.multiple_of(half * HALF + n, STEP), STEP)]
            out = (x.astype(F32) - update).astype(BF)
            out_ref[i, :, n : n + STEP] = out
            wide = out.astype(F32)
            squares[n // STEP] += jnp.sum(wide * wide, axis=0, keepdims=True)
        stores.append(load(out_ref.at[i], out_hbm.at[rows, columns], sems.at[i]))
    squares = jnp.concatenate(squares, axis=1)
    if flip:
        for r in range(2 * CHIPS):
            sq_ref[r, :, columns] = squares
            sq_ref[r, :, pl.ds(pl.multiple_of((1 - half) * HALF, HALF), HALF)] = refs[1][...]
    else:
        sq_ref[...] = squares
    for store in stores:
        store.wait()


def update(flip, eigvecs, reflectors, scaled, *so_far):
    rows, columns = eigvecs.shape
    blocks = 3
    in_specs = [VMEM] * 3
    args = [eigvecs, reflectors, scaled]
    aliases = {}
    squares = (1, HALF)
    if flip:
        in_specs += [HBM, VMEM]
        args += so_far
        aliases = {3: 0}
        squares = (2 * CHIPS, 1, columns)
    return call(
        functools.partial(update_kernel, flip),
        (
            jax.ShapeDtypeStruct((rows, columns), BF),
            jax.ShapeDtypeStruct(squares, F32),
        ),
        in_specs,
        (HBM, VMEM),
        2 * rows * HALF * PANELS * WIDTH,
        6 * 2**20,
        input_output_aliases=aliases,
        scratch_shapes=[
            pltpu.VMEM((blocks, rows // blocks, HALF), BF),
            pltpu.SemaphoreType.DMA((blocks,)),
        ],
    )(*args)


def swapped(value):
    return lax.ppermute(value, "core", [(0, 1), (1, 0)])


def exchanged(value, axes):
    return lax.all_to_all(value, axes, split_axis=0, concat_axis=0, tiled=True)


def steps(eigvecs, reflectors, factors):
    rows = eigvecs.shape[0]
    flops = 2 * rows * HALF * PANELS * WIDTH
    chunks = jax.ShapeDtypeStruct((CHIPS, CHUNK, WIDTH), BF)
    projections = jax.ShapeDtypeStruct((CHIPS, PROJ, WIDTH), BF)
    other, gram, eigvecs, reflectors = call(
        first_kernel,
        (
            chunks,
            jax.ShapeDtypeStruct((CHIPS, SHARE, WIDTH), BF),
            pltpu.VMEM(eigvecs.shape, BF),
            pltpu.VMEM(reflectors.shape, BF),
        ),
        [HBM] * 2,
        (VMEM,) * 4,
        2 * flops,
        8 * 2**20,
        limit=54,
        scratch_shapes=[
            pltpu.VMEM((PAIRS * WIDTH, WIDTH), BF),
            pltpu.SemaphoreType.DMA((2 * HALF // STEP,)),
            pltpu.SemaphoreType.DMA((PANELS,)),
        ],
    )(eigvecs, reflectors)
    other = swapped(other)
    own = call(own_kernel, projections, [VMEM] * 2, VMEM, flops, 6 * 2**20)(
        eigvecs, reflectors
    )
    payload = call(combine_kernel, chunks, [VMEM] * 3, VMEM, 2**20, 4 * 2**20)(own, gram, other)
    parts = exchanged(payload, CHIP)
    sums = call(sum_kernel, chunks, [VMEM], VMEM, 2**20, 3 * 2**20)(parts)
    mine = exchanged(sums, CHIP)
    theirs = swapped(mine[:, PROJ:, :])
    scaled = call(
        solve_kernel,
        projections,
        [VMEM] * 3,
        VMEM,
        2**28,
        4 * 2**20,
        scratch_shapes=[pltpu.VMEM((PAIRS * WIDTH, WIDTH), BF)],
    )(mine, theirs, factors)
    scaled_theirs = swapped(scaled)
    vectors, squares_mine = update(False, eigvecs, reflectors, scaled)
    vectors, squares = update(
        True, eigvecs, reflectors, scaled_theirs, vectors, squares_mine
    )
    everything = exchanged(squares, ROW)
    deviation = jnp.sqrt(jnp.sum(everything, axis=(0, 1)) / NORD) - 1.0
    return (vectors, deviation)


def solution(mesh):
    split_mesh = Mesh(mesh.devices.reshape(4, 4, 2, 4), ("x", "z", "core", "col"))
    placed = (P(ROW, "col"), P(None, ROW, None), P())
    return jax.shard_map(
        steps, mesh=split_mesh, in_specs=placed, out_specs=(P(ROW, "col"), P("col")), check_vma=False
    )
```

```python
import functools

import jax
import jax.numpy as jnp
from jax import lax
from jax.experimental import pallas as pl
from jax.experimental.pallas import tpu as pltpu
from jax.sharding import Mesh
from jax.sharding import PartitionSpec as P

NORD = 49152
WIDTH = 128
PANELS = 8
CHIPS = 16
OWN = 32
HALF = CHIPS * OWN
PAIRS = PANELS * (PANELS - 1) // 2
BLOCKS = PAIRS + PANELS // 2
SHARE = BLOCKS * WIDTH // (2 * CHIPS)
PROJ = PANELS * OWN
MORE = PROJ + SHARE
TILE = 16
CHUNK = MORE + TILE
STEP = 256
BF = jnp.bfloat16
F32 = jnp.float32
CHIP = ("x", "z")
ROW = (*CHIP, "core")
VMEM = pl.BlockSpec(memory_space=pltpu.VMEM)
HBM = pl.BlockSpec(memory_space=pltpu.HBM)


def call(kernel, out_shape, in_specs, out_specs, flops, nbytes, limit=12, **kw):
    return pl.pallas_call(
        kernel,
        out_shape=out_shape,
        in_specs=in_specs,
        out_specs=out_specs,
        compiler_params=pltpu.CompilerParams(vmem_limit_bytes=limit * 2**20),
        cost_estimate=pl.CostEstimate(flops=flops, bytes_accessed=nbytes, transcendentals=0),
        **kw,
    )


def first_block(k):
    return k * (k - 1) // 2


def load(source, target, sem):
    copy = pltpu.make_async_copy(source, target, sem)
    copy.start()
    return copy


def pair(v_ref, k):
    return jnp.concatenate([v_ref[k], v_ref[k + 1]], axis=1)


def parts_of(value):
    parts = []
    for _ in range(3):
        part = value.astype(BF).astype(F32)
        parts.append(part)
        value = value - part
    return parts


def packed(values):
    row = lax.broadcasted_iota(jnp.int32, (TILE, WIDTH), 0)
    tile = jnp.zeros((TILE, WIDTH), F32)
    for i, value in enumerate(values):
        for j, part in enumerate(parts_of(value)):
            tile = jnp.where(row == 3 * i + j, part, tile)
    return tile.astype(BF)


def unpacked(tile, count):
    tile = tile.astype(F32)
    return [
        tile[3 * i : 3 * i + 1] + tile[3 * i + 1 : 3 * i + 2] + tile[3 * i + 2 : 3 * i + 3]
        for i in range(count)
    ]


def project(x_ref, v_ref, half, p_ref, ready=None):
    squares = []
    for n in range(0, HALF, STEP):
        if ready is not None:
            ready(n // STEP)
        x = x_ref[:, pl.ds(pl.multiple_of(half * HALF + n, STEP), STEP)]
        wide = x.astype(F32)
        squares.append(jnp.sum(wide * wide, axis=0, keepdims=True))
        xt = x.T
        chips = slice(n // OWN, (n + STEP) // OWN)
        for k in range(0, PANELS, 2):
            both = jnp.dot(xt, pair(v_ref, k), preferred_element_type=F32).astype(BF)
            for dk in range(2):
                p_ref[chips, (k + dk) * OWN : (k + dk + 1) * OWN, :] = both[
                    :, dk * WIDTH : (dk + 1) * WIDTH
                ].reshape(STEP // OWN, OWN, WIDTH)
    return jnp.concatenate(squares, axis=1)


def load_half(half, x_hbm, x_ref, sems):
    copies = []
    for n in range(0, HALF, STEP):
        at = pl.ds(pl.multiple_of(half * HALF + n, STEP), STEP)
        copies.append(load(x_hbm.at[:, at], x_ref.at[:, at], sems.at[n // STEP]))
    return copies


def group_of(values, s):
    at = s * OWN // WIDTH * WIDTH
    return values[:, at : at + WIDTH]


def first_kernel(
    x_hbm, v_hbm, other_ref, mine_ref, diag_ref, x_ref, v_ref, g_ref, x_sems, v_sems
):
    core = lax.axis_index("core")
    v_copies = [load(v_hbm.at[k], v_ref.at[k], v_sems.at[k]) for k in range(PANELS)]
    x_copies = load_half(1 - core, x_hbm, x_ref, x_sems.at[0])
    own_copies = load_half(core, x_hbm, x_ref, x_sems.at[1])
    row = lax.broadcasted_iota(jnp.int32, (WIDTH, WIDTH), 0)
    column = lax.broadcasted_iota(jnp.int32, (WIDTH, WIDTH), 1)
    diag = []
    for k in range(0, PANELS, 2):
        v_copies[k].wait()
        v_copies[k + 1].wait()
        right = pair(v_ref, k)
        for j in range(0, k + 1, 2):
            both = jnp.dot(pair(v_ref, j).T, right, preferred_element_type=F32)
            blocks = [
                [
                    both[dj * WIDTH : (dj + 1) * WIDTH, dk * WIDTH : (dk + 1) * WIDTH]
                    for dk in range(2)
                ]
                for dj in range(2)
            ]
            for dj in range(2):
                for dk in range(2):
                    if j + dj < k + dk:
                        at = (first_block(k + dk) + j + dj) * WIDTH
                        g_ref[at : at + WIDTH, :] = blocks[dj][dk].astype(BF)
            if j == k:
                at = (PAIRS + k // 2) * WIDTH
                g_ref[at : at + WIDTH, :] = jnp.where(
                    row < column, blocks[0][0], blocks[1][1]
                ).astype(BF)
                for d in range(2):
                    diag.append(
                        jnp.sum(
                            jnp.where(row == column, blocks[d][d], 0.0), axis=0, keepdims=True
                        )
                    )
    for k in range(PANELS):
        diag_ref[k : k + 1, :] = diag[k]
    for s in range(CHIPS):
        at = pl.multiple_of((1 - core) * CHIPS * SHARE + s * SHARE, 16)
        other_ref[s, PROJ:MORE, :] = g_ref[pl.ds(at, SHARE), :]
        at = pl.multiple_of(core * CHIPS * SHARE + s * SHARE, 16)
        mine_ref[s] = g_ref[pl.ds(at, SHARE), :]
    squares = project(x_ref, v_ref, 1 - core, other_ref, lambda n: x_copies[n].wait())
    for s in range(CHIPS):
        other_ref[s, MORE:, :] = packed([group_of(squares, s), diag[s % PANELS]])
    for copy in own_copies:
        copy.wait()


def own_kernel(x_ref, v_ref, p_ref, sq_ref):
    sq_ref[...] = project(x_ref, v_ref, lax.axis_index("core"), p_ref)


def combine_kernel(own_ref, sq_ref, gram_ref, diag_ref, other_ref, out_ref):
    for s in range(CHIPS):
        out_ref[s, :PROJ, :] = (
            own_ref[s].astype(F32) + other_ref[s, :PROJ, :].astype(F32)
        ).astype(BF)
        out_ref[s, PROJ:MORE, :] = (
            gram_ref[s].astype(F32) + other_ref[s, PROJ:MORE, :].astype(F32)
        ).astype(BF)
        squares, diag = unpacked(other_ref[s, MORE:, :], 2)
        k = s % PANELS
        out_ref[s, MORE:, :] = packed(
            [group_of(sq_ref[...], s) + squares, diag_ref[k : k + 1, :] + diag]
        )


def sum_kernel(parts_ref, out_ref):
    for at in range(0, MORE, TILE):
        total = parts_ref[0, at : at + TILE, :].astype(F32)
        for s in range(1, CHIPS):
            total = total + parts_ref[s, at : at + TILE, :].astype(F32)
        total = total.astype(BF)
        for s in range(CHIPS):
            out_ref[s, at : at + TILE, :] = total
    total = parts_ref[0, MORE:, :].astype(F32)
    for s in range(1, CHIPS):
        total = total + parts_ref[s, MORE:, :].astype(F32)
    tile = packed(unpacked(total, 2))
    for s in range(CHIPS):
        out_ref[s, MORE:, :] = tile


def split(value):
    high = value.astype(BF)
    return high, (value - high.astype(F32)).astype(BF)


def solve_kernel(mine_ref, theirs_ref, t_ref, out_ref, dev_ref, g_ref):
    core = lax.axis_index("core")
    for s in range(CHIPS):
        at = pl.multiple_of(core * CHIPS * SHARE + s * SHARE, 16)
        g_ref[pl.ds(at, SHARE), :] = mine_ref[s, PROJ:MORE, :]
        at = pl.multiple_of((1 - core) * CHIPS * SHARE + s * SHARE, 16)
        g_ref[pl.ds(at, SHARE), :] = theirs_ref[s]
    row = lax.broadcasted_iota(jnp.int32, (WIDTH, WIDTH), 0)
    column = lax.broadcasted_iota(jnp.int32, (WIDTH, WIDTH), 1)
    groups = range(0, CHIPS, CHIPS // 2)
    done = [[] for _ in groups]
    change = [jnp.zeros((HALF // 2, WIDTH), F32) for _ in groups]
    for k in range(PANELS):
        rows = slice(k * OWN, (k + 1) * OWN)
        factor, rest = split(t_ref[k])
        factor = jnp.concatenate([factor, factor, rest], axis=1)
        at = (PAIRS + k // 2) * WIDTH
        own = g_ref[at : at + WIDTH, :].astype(F32)
        own = jnp.where(row > column if k % 2 else row < column, 2.0 * own, 0.0).astype(BF)
        diag = unpacked(mine_ref[k, MORE:, :], 2)[1]
        for i, g in enumerate(groups):
            chips = slice(g, g + CHIPS // 2)
            proj = mine_ref[chips, rows, :].reshape(HALF // 2, WIDTH).astype(F32)
            if k:
                at = first_block(k) * WIDTH
                cross = g_ref[at : at + k * WIDTH, :]
                before = jnp.concatenate(done[i], axis=1) if k > 1 else done[i][0]
                proj = proj - jnp.dot(before, cross, preferred_element_type=F32)
            high, low = split(proj)
            scaled = lax.dot_general(
                jnp.concatenate([high, low, high], axis=1),
                factor,
                (((1,), (1,)), ((), ())),
                preferred_element_type=F32,
            ).astype(BF)
            done[i].append(scaled)
            out_ref[chips, rows, :] = scaled.reshape(CHIPS // 2, OWN, WIDTH)
            wide = scaled.astype(F32)
            change[i] += wide * (
                jnp.dot(scaled, own, preferred_element_type=F32) + wide * diag - 2.0 * proj
            )
    squares = jnp.concatenate(
        [jnp.sum(part.T, axis=0, keepdims=True) for part in change], axis=1
    )
    before = jnp.concatenate(
        [
            unpacked(mine_ref[s, MORE:, :], 2)[0]
            for s in range(0, CHIPS, WIDTH // OWN)
        ],
        axis=1,
    )
    deviation = jnp.sqrt(jnp.maximum(before + squares, 0.0) / NORD) - 1.0
    dev_ref[...] = deviation
    tile = packed([deviation[:, n : n + WIDTH] for n in range(0, HALF, WIDTH)])
    for s in range(CHIPS):
        out_ref[s, PROJ:, :] = tile


def update_kernel(flip, x_ref, v_ref, s_ref, *refs):
    half = lax.axis_index("core")
    if flip:
        _, dev_ref, out_hbm, both_ref, out_ref, sems = refs
        columns = pl.ds(pl.multiple_of(half * HALF, HALF), HALF)
        both_ref[:, columns] = dev_ref[...]
        half = 1 - half
        columns = pl.ds(pl.multiple_of(half * HALF, HALF), HALF)
        both_ref[:, columns] = jnp.concatenate(
            unpacked(s_ref[0, PROJ:, :], HALF // WIDTH), axis=1
        )
    else:
        out_hbm, out_ref, sems = refs
        columns = pl.ds(pl.multiple_of(half * HALF, HALF), HALF)
    blocks, block = out_ref.shape[:2]
    stores = []
    for i in range(blocks):
        rows = slice(i * block, (i + 1) * block)
        left = jnp.concatenate([v_ref[k, rows, :] for k in range(PANELS)], axis=1)
        for n in range(0, HALF, STEP):
            chips = slice(n // OWN, (n + STEP) // OWN)
            right = jnp.concatenate(
                [
                    s_ref[chips, k * OWN : (k + 1) * OWN, :].reshape(STEP, WIDTH)
                    for k in range(PANELS)
                ],
                axis=1,
            )
            update = lax.dot_general(
                left, right, (((1,), (1,)), ((), ())), preferred_element_type=F32
            )
            x = x_ref[rows, pl.ds(pl.multiple_of(half * HALF + n, STEP), STEP)]
            out_ref[i, :, n : n + STEP] = (x.astype(F32) - update).astype(BF)
        stores.append(load(out_ref.at[i], out_hbm.at[rows, columns], sems.at[i]))
    for store in stores:
        store.wait()


def update(flip, eigvecs, reflectors, scaled, *so_far):
    rows = eigvecs.shape[0]
    blocks = 3
    in_specs = [VMEM] * 3
    out_shape = jax.ShapeDtypeStruct(eigvecs.shape, BF)
    out_specs = HBM
    aliases = {}
    if flip:
        in_specs += [HBM, VMEM]
        aliases = {3: 0}
        out_shape = (out_shape, jax.ShapeDtypeStruct((1, 2 * HALF), F32))
        out_specs = (HBM, VMEM)
    return call(
        functools.partial(update_kernel, flip),
        out_shape,
        in_specs,
        out_specs,
        2 * rows * HALF * PANELS * WIDTH,
        6 * 2**20,
        input_output_aliases=aliases,
        scratch_shapes=[
            pltpu.VMEM((blocks, rows // blocks, HALF), BF),
            pltpu.SemaphoreType.DMA((blocks,)),
        ],
    )(eigvecs, reflectors, scaled, *so_far)


def swapped(value):
    return lax.ppermute(value, "core", [(0, 1), (1, 0)])


def exchanged(value, axes):
    return lax.all_to_all(value, axes, split_axis=0, concat_axis=0, tiled=True)


def steps(eigvecs, reflectors, factors):
    rows = eigvecs.shape[0]
    flops = 2 * rows * HALF * PANELS * WIDTH
    chunks = jax.ShapeDtypeStruct((CHIPS, CHUNK, WIDTH), BF)
    tiles = HALF // STEP
    other, gram, diag, eigvecs, reflectors = call(
        first_kernel,
        (
            chunks,
            jax.ShapeDtypeStruct((CHIPS, SHARE, WIDTH), BF),
            jax.ShapeDtypeStruct((PANELS, WIDTH), F32),
            pltpu.VMEM(eigvecs.shape, BF),
            pltpu.VMEM(reflectors.shape, BF),
        ),
        [HBM] * 2,
        (VMEM,) * 5,
        2 * flops,
        8 * 2**20,
        limit=54,
        scratch_shapes=[
            pltpu.VMEM((BLOCKS * WIDTH, WIDTH), BF),
            pltpu.SemaphoreType.DMA((2, tiles)),
            pltpu.SemaphoreType.DMA((PANELS,)),
        ],
    )(eigvecs, reflectors)
    other = swapped(other)
    own, squares = call(
        own_kernel,
        (
            jax.ShapeDtypeStruct((CHIPS, PROJ, WIDTH), BF),
            jax.ShapeDtypeStruct((1, HALF), F32),
        ),
        [VMEM] * 2,
        (VMEM,) * 2,
        flops,
        6 * 2**20,
    )(eigvecs, reflectors)
    payload = call(combine_kernel, chunks, [VMEM] * 5, VMEM, 2**20, 4 * 2**20)(
        own, squares, gram, diag, other
    )
    parts = exchanged(payload, CHIP)
    sums = call(sum_kernel, chunks, [VMEM], VMEM, 2**20, 3 * 2**20)(parts)
    mine = exchanged(sums, CHIP)
    theirs = swapped(mine[:, PROJ:MORE, :])
    scaled, dev = call(
        solve_kernel,
        (
            jax.ShapeDtypeStruct((CHIPS, PROJ + TILE, WIDTH), BF),
            jax.ShapeDtypeStruct((1, HALF), F32),
        ),
        [VMEM] * 3,
        (VMEM,) * 2,
        2**28,
        4 * 2**20,
        scratch_shapes=[pltpu.VMEM((BLOCKS * WIDTH, WIDTH), BF)],
    )(mine, theirs, factors)
    scaled_theirs = swapped(scaled)
    vectors = update(False, eigvecs, reflectors, scaled)
    vectors, deviation = update(True, eigvecs, reflectors, scaled_theirs, vectors, dev)
    return (vectors, deviation.reshape(-1))


def solution(mesh):
    split_mesh = Mesh(mesh.devices.reshape(4, 4, 2, 4), ("x", "z", "core", "col"))
    placed = (P(ROW, "col"), P(None, ROW, None), P())
    return jax.shard_map(
        steps, mesh=split_mesh, in_specs=placed, out_specs=(P(ROW, "col"), P("col")), check_vma=False
    )
```

```python
import functools

import jax
import jax.numpy as jnp
from jax import lax
from jax.experimental import pallas as pl
from jax.experimental.pallas import tpu as pltpu
from jax.sharding import PartitionSpec as P

NORD = 49152
WIDTH = 128
PANELS = 8
CHIPS = 16
OWN = 32
HALF = CHIPS * OWN
PAIRS = PANELS * (PANELS - 1) // 2
BLOCKS = PAIRS + PANELS // 2
SHARE = BLOCKS * WIDTH // (2 * CHIPS)
PROJ = PANELS * OWN
MORE = PROJ + SHARE
TILE = 16
CHUNK = MORE + TILE
STEP = 256
AHEAD = 2
BF = jnp.bfloat16
F32 = jnp.float32
SIDE = 4


def device(x, z, core):
    return (x * SIDE + z) * 2 + core


def lines(along_z):
    along_x = [[device(x, z, 1 - along_z) for x in range(SIDE)] for z in range(SIDE)]
    return [[device(x, z, along_z) for z in range(SIDE)] for x in range(SIDE)] + along_x


WIDE, NARROW = lines(0), lines(1)
VMEM = pl.BlockSpec(memory_space=pltpu.VMEM)
HBM = pl.BlockSpec(memory_space=pltpu.HBM)


def call(kernel, out_shape, in_specs, out_specs, flops, nbytes, limit=12, **kw):
    return pl.pallas_call(
        kernel,
        out_shape=out_shape,
        in_specs=in_specs,
        out_specs=out_specs,
        compiler_params=pltpu.CompilerParams(vmem_limit_bytes=limit * 2**20),
        cost_estimate=pl.CostEstimate(flops=flops, bytes_accessed=nbytes, transcendentals=0),
        **kw,
    )


def core_index():
    return lax.rem(lax.axis_index("row"), 2)


def first_block(k):
    return k * (k - 1) // 2


def load(source, target, sem):
    copy = pltpu.make_async_copy(source, target, sem)
    copy.start()
    return copy


def pair(v_ref, k):
    return jnp.concatenate([v_ref[k], v_ref[k + 1]], axis=1)


def parts_of(value):
    parts = []
    for _ in range(3):
        part = value.astype(BF).astype(F32)
        parts.append(part)
        value = value - part
    return parts


def packed(values):
    row = lax.broadcasted_iota(jnp.int32, (TILE, WIDTH), 0)
    tile = jnp.zeros((TILE, WIDTH), F32)
    for i, value in enumerate(values):
        for j, part in enumerate(parts_of(value)):
            tile = jnp.where(row == 3 * i + j, part, tile)
    return tile.astype(BF)


def unpacked(tile, count):
    tile = tile.astype(F32)
    return [
        tile[3 * i : 3 * i + 1] + tile[3 * i + 1 : 3 * i + 2] + tile[3 * i + 2 : 3 * i + 3]
        for i in range(count)
    ]


def squares_of(x):
    wide = x.astype(F32)
    return jnp.sum(wide * wide, axis=0, keepdims=True)


def put(p_ref, n, k, both):
    chips = slice(n // OWN, (n + STEP) // OWN)
    for dk in range(2):
        p_ref[chips, (k + dk) * OWN : (k + dk + 1) * OWN, :] = (
            both[:, dk * WIDTH : (dk + 1) * WIDTH].astype(BF).reshape(STEP // OWN, OWN, WIDTH)
        )


def project(x_ref, v_ref, half, p_ref):
    squares = []
    for n in range(0, HALF, STEP):
        x = x_ref[:, pl.ds(pl.multiple_of(half * HALF + n, STEP), STEP)]
        squares.append(squares_of(x))
        xt = x.T
        for k in range(0, PANELS, 2):
            put(p_ref, n, k, jnp.dot(xt, pair(v_ref, k), preferred_element_type=F32))
    return jnp.concatenate(squares, axis=1)


def group_of(values, s):
    at = s * OWN // WIDTH * WIDTH
    return values[:, at : at + WIDTH]


def first_kernel(
    x_hbm, v_hbm, other_ref, mine_ref, diag_ref, x_ref, v_ref, xt_ref, vt_ref, sems
):
    core = core_index()
    half = 1 - core

    def columns(half, n):
        return pl.ds(pl.multiple_of(half * HALF + n * STEP, STEP), STEP)

    def of_x(half, n):
        at = columns(half, n)
        return x_hbm.at[:, at], x_ref.at[:, at]

    def of_v(k):
        return v_hbm.at[2 * k : 2 * k + 2], v_ref.at[2 * k : 2 * k + 2]

    queue = [of_x(half, 0), of_v(0), of_v(1), of_x(half, 1), of_v(2), of_v(3)]
    queue += [of_x(core, 0), of_x(core, 1)]
    copies = []

    def start():
        if len(copies) < len(queue):
            copies.append(load(*queue[len(copies)], sems.at[len(copies)]))

    def arrived(i):
        copies[i].wait()
        start()

    for _ in range(AHEAD):
        start()
    row = lax.broadcasted_iota(jnp.int32, (WIDTH, WIDTH), 0)
    column = lax.broadcasted_iota(jnp.int32, (WIDTH, WIDTH), 1)
    squares = [None] * (HALF // STEP)
    diag = []

    def turn(n):
        x = x_ref[:, columns(half, n)]
        xt_ref[n] = x.T
        squares[n] = squares_of(x)

    def product(n, k):
        put(
            other_ref,
            n * STEP,
            2 * k,
            jnp.dot(xt_ref[n], pair(v_ref, 2 * k), preferred_element_type=F32),
        )

    def keep(block, value):
        sent = core != block // CHIPS
        value = value.astype(BF)
        spot = block % CHIPS
        other_ref[jnp.where(sent, spot, CHIPS), PROJ:MORE, :] = value
        mine_ref[jnp.where(sent, CHIPS, spot)] = value

    def gram(j, k):
        both = jnp.dot(vt_ref[j], pair(v_ref, 2 * k), preferred_element_type=F32)
        blocks = [
            [both[d * WIDTH : (d + 1) * WIDTH, e * WIDTH : (e + 1) * WIDTH] for e in range(2)]
            for d in range(2)
        ]
        for d in range(2):
            for e in range(2):
                if 2 * j + d < 2 * k + e:
                    keep(first_block(2 * k + e) + 2 * j + d, blocks[d][e])
        if j == k:
            keep(PAIRS + k, jnp.where(row < column, blocks[0][0], blocks[1][1]))
            for d in range(2):
                own = jnp.where(row == column, blocks[d][d], 0.0)
                diag.append(jnp.sum(own, axis=0, keepdims=True))

    def panels(k, tiles):
        vt_ref[k] = pair(v_ref, 2 * k).T
        for n in tiles:
            product(n, k)
        for j in range(k + 1):
            gram(j, k)

    arrived(0)
    turn(0)
    arrived(1)
    panels(0, [0])
    arrived(2)
    panels(1, [0])
    arrived(3)
    turn(1)
    product(1, 0)
    product(1, 1)
    arrived(4)
    panels(2, [0, 1])
    arrived(5)
    panels(3, [0, 1])
    squares = jnp.concatenate(squares, axis=1)
    for k in range(PANELS):
        diag_ref[k : k + 1, :] = diag[k]
    for s in range(CHIPS):
        other_ref[s, MORE:, :] = packed([group_of(squares, s), diag[s % PANELS]])
    arrived(6)
    arrived(7)


def own_kernel(x_ref, v_ref, p_ref, sq_ref):
    sq_ref[...] = project(x_ref, v_ref, core_index(), p_ref)


def combine_kernel(own_ref, sq_ref, gram_ref, diag_ref, other_ref, out_ref):
    for s in range(CHIPS):
        out_ref[s, :PROJ, :] = (
            own_ref[s].astype(F32) + other_ref[s, :PROJ, :].astype(F32)
        ).astype(BF)
        out_ref[s, PROJ:MORE, :] = (
            gram_ref[s].astype(F32) + other_ref[s, PROJ:MORE, :].astype(F32)
        ).astype(BF)
        squares, diag = unpacked(other_ref[s, MORE:, :], 2)
        k = s % PANELS
        out_ref[s, MORE:, :] = packed(
            [group_of(sq_ref[...], s) + squares, diag_ref[k : k + 1, :] + diag]
        )


def sum_kernel(parts_ref, out_ref):
    senders, rows = parts_ref.shape[:2]
    chunks = rows // CHUNK
    for i in range(chunks):
        for at in range(0, CHUNK, TILE):
            here = slice(i * CHUNK + at, i * CHUNK + at + TILE)
            total = parts_ref[0, here, :].astype(F32)
            for s in range(1, senders):
                total = total + parts_ref[s, here, :].astype(F32)
            total = packed(unpacked(total, 2)) if at == MORE else total.astype(BF)
            for s in range(i, SIDE, chunks):
                out_ref[s, at : at + TILE, :] = total


def spread_kernel(chunks_ref, out_ref):
    for j in range(SIDE):
        for i in range(SIDE):
            out_ref[j, i * CHUNK : (i + 1) * CHUNK, :] = chunks_ref[i]


def split(value):
    high = value.astype(BF)
    return high, (value - high.astype(F32)).astype(BF)


def solve_kernel(mine_ref, theirs_ref, t_ref, out_ref, dev_ref, g_ref):
    core = core_index()
    for s in range(CHIPS):
        at = pl.multiple_of(core * CHIPS * SHARE + s * SHARE, 16)
        g_ref[pl.ds(at, SHARE), :] = mine_ref[s, PROJ:MORE, :]
        at = pl.multiple_of((1 - core) * CHIPS * SHARE + s * SHARE, 16)
        g_ref[pl.ds(at, SHARE), :] = theirs_ref[s]
    row = lax.broadcasted_iota(jnp.int32, (WIDTH, WIDTH), 0)
    column = lax.broadcasted_iota(jnp.int32, (WIDTH, WIDTH), 1)
    done = []
    change = jnp.zeros((HALF, WIDTH), F32)
    for k in range(PANELS + 1):
        rows = slice(k * OWN, (k + 1) * OWN)
        if k:
            at = (PAIRS + (k - 1) // 2) * WIDTH
            own = g_ref[at : at + WIDTH, :].astype(F32)
            own = jnp.where(row < column if k % 2 else row > column, 2.0 * own, 0.0).astype(BF)
            if k > 1:
                own = jnp.concatenate([jnp.zeros(((k - 1) * WIDTH, WIDTH), BF), own], axis=0)
            right = own
            if k < PANELS:
                at = first_block(k) * WIDTH
                right = jnp.concatenate([g_ref[at : at + k * WIDTH, :], own], axis=1)
            else:
                right, done = own[-WIDTH:], done[-1:]
            before = jnp.concatenate(done, axis=1) if len(done) > 1 else done[0]
            both = jnp.dot(before, right, preferred_element_type=F32)
            change += done[-1].astype(F32) * both[:, -WIDTH:]
        if k == PANELS:
            break
        proj = mine_ref[:, rows, :].reshape(HALF, WIDTH).astype(F32)
        if k:
            proj = proj - both[:, :WIDTH]
        factor, rest = split(t_ref[k])
        high, low = split(proj)
        scaled = lax.dot_general(
            jnp.concatenate([high, low, high], axis=1),
            jnp.concatenate([factor, factor, rest], axis=1),
            (((1,), (1,)), ((), ())),
            preferred_element_type=F32,
        ).astype(BF)
        done.append(scaled)
        out_ref[:, rows, :] = scaled.reshape(CHIPS, OWN, WIDTH)
        wide = scaled.astype(F32)
        change += wide * (wide * unpacked(mine_ref[k, MORE:, :], 2)[1] - 2.0 * proj)
    squares = jnp.sum(change.T, axis=0, keepdims=True)
    before = jnp.concatenate(
        [
            unpacked(mine_ref[s, MORE:, :], 2)[0]
            for s in range(0, CHIPS, WIDTH // OWN)
        ],
        axis=1,
    )
    deviation = jnp.sqrt(jnp.maximum(before + squares, 0.0) / NORD) - 1.0
    dev_ref[...] = deviation
    tile = packed([deviation[:, n : n + WIDTH] for n in range(0, HALF, WIDTH)])
    for s in range(CHIPS):
        out_ref[s, PROJ:, :] = tile


def update_kernel(flip, x_ref, v_ref, s_ref, *refs):
    out_hbm, *more, out_ref, sems = refs[2:] if flip else refs
    core = core_index()
    half = 1 - core if flip else core
    left = jnp.concatenate([v_ref[k] for k in range(PANELS)], axis=1)
    stores = []
    for n in range(0, HALF, STEP):
        chips = slice(n // OWN, (n + STEP) // OWN)
        right = jnp.concatenate(
            [s_ref[chips, k * OWN : (k + 1) * OWN, :].reshape(STEP, WIDTH) for k in range(PANELS)],
            axis=1,
        )
        update = lax.dot_general(left, right, (((1,), (1,)), ((), ())), preferred_element_type=F32)
        columns = pl.ds(pl.multiple_of(half * HALF + n, STEP), STEP)
        i = n // STEP
        out_ref[i] = (x_ref[:, columns].astype(F32) - update).astype(BF)
        stores.append(load(out_ref.at[i], out_hbm.at[:, columns], sems.at[i]))
    if flip:
        theirs = jnp.concatenate(unpacked(s_ref[0, PROJ:, :], HALF // WIDTH), axis=1)
        more[0][:, pl.ds(pl.multiple_of(core * HALF, HALF), HALF)] = refs[1][...]
        more[0][:, pl.ds(pl.multiple_of(half * HALF, HALF), HALF)] = theirs
    for store in stores:
        store.wait()


def update(flip, eigvecs, reflectors, scaled, *so_far):
    rows = eigvecs.shape[0]
    tiles = HALF // STEP
    in_specs = [VMEM] * 3
    out_shape = jax.ShapeDtypeStruct(eigvecs.shape, BF)
    out_specs = HBM
    aliases = {}
    if flip:
        in_specs += [HBM, VMEM]
        aliases = {3: 0}
        out_shape = (out_shape, jax.ShapeDtypeStruct((1, 2 * HALF), F32))
        out_specs = (HBM, VMEM)
    return call(
        functools.partial(update_kernel, flip),
        out_shape,
        in_specs,
        out_specs,
        2 * rows * HALF * PANELS * WIDTH,
        6 * 2**20,
        input_output_aliases=aliases,
        scratch_shapes=[
            pltpu.VMEM((tiles, rows, STEP), BF),
            pltpu.SemaphoreType.DMA((tiles,)),
        ],
    )(eigvecs, reflectors, scaled, *so_far)


def swapped(value):
    pairs = [(i ^ 1, i) for i in range(2 * CHIPS)]
    return lax.ppermute(value, "row", pairs)


def exchanged(value, groups):
    return lax.all_to_all(
        value, "row", split_axis=0, concat_axis=0, axis_index_groups=groups, tiled=True
    )


def steps(eigvecs, reflectors, factors):
    rows = eigvecs.shape[0]
    flops = 2 * rows * HALF * PANELS * WIDTH
    chunks = jax.ShapeDtypeStruct((CHIPS, CHUNK, WIDTH), BF)
    tiles = HALF // STEP
    other, gram, diag, eigvecs, reflectors = call(
        first_kernel,
        (
            jax.ShapeDtypeStruct((CHIPS + 1, CHUNK, WIDTH), BF),
            jax.ShapeDtypeStruct((CHIPS + 1, SHARE, WIDTH), BF),
            jax.ShapeDtypeStruct((PANELS, WIDTH), F32),
            pltpu.VMEM(eigvecs.shape, BF),
            pltpu.VMEM(reflectors.shape, BF),
        ),
        [HBM] * 2,
        (VMEM,) * 5,
        2 * flops,
        8 * 2**20,
        limit=54,
        scratch_shapes=[
            pltpu.VMEM((tiles, STEP, rows), BF),
            pltpu.VMEM((PANELS // 2, 2 * WIDTH, rows), BF),
            pltpu.SemaphoreType.DMA((2 * tiles + PANELS // 2,)),
        ],
    )(eigvecs, reflectors)
    other = swapped(other)
    own, squares = call(
        own_kernel,
        (
            jax.ShapeDtypeStruct((CHIPS, PROJ, WIDTH), BF),
            jax.ShapeDtypeStruct((1, HALF), F32),
        ),
        [VMEM] * 2,
        (VMEM,) * 2,
        flops,
        6 * 2**20,
    )(eigvecs, reflectors)
    payload = call(combine_kernel, chunks, [VMEM] * 5, VMEM, 2**20, 4 * 2**20)(
        own, squares, gram, diag, other
    )
    lot = jax.ShapeDtypeStruct((SIDE, CHUNK, WIDTH), BF)
    lots = jax.ShapeDtypeStruct((SIDE, SIDE * CHUNK, WIDTH), BF)
    for groups in (WIDE, NARROW):
        parts = exchanged(payload.reshape(SIDE, -1, WIDTH), groups)
        payload = call(sum_kernel, lot, [VMEM], VMEM, 2**20, 2 * 2**20)(parts)
    gathered = exchanged(payload, NARROW)
    gathered = call(spread_kernel, lots, [VMEM], VMEM, 2**20, 2 * 2**20)(gathered)
    mine = exchanged(gathered, WIDE).reshape(CHIPS, CHUNK, WIDTH)
    theirs = swapped(mine[:, PROJ:MORE, :])
    scaled, dev = call(
        solve_kernel,
        (
            jax.ShapeDtypeStruct((CHIPS, PROJ + TILE, WIDTH), BF),
            jax.ShapeDtypeStruct((1, HALF), F32),
        ),
        [VMEM] * 3,
        (VMEM,) * 2,
        2**28,
        4 * 2**20,
        scratch_shapes=[pltpu.VMEM((BLOCKS * WIDTH, WIDTH), BF)],
    )(mine, theirs, factors)
    scaled_theirs = swapped(scaled)
    vectors = update(False, eigvecs, reflectors, scaled)
    vectors, deviation = update(True, eigvecs, reflectors, scaled_theirs, vectors, dev)
    return (vectors, deviation.reshape(-1))


def solution(mesh):
    placed = (P("row", "col"), P(None, "row", None), P())
    return jax.shard_map(
        steps, mesh=mesh, in_specs=placed, out_specs=(P("row", "col"), P("col")), check_vma=False
    )
```

```python
import functools

import jax
import jax.numpy as jnp
from jax import lax
from jax.experimental import pallas as pl
from jax.experimental.pallas import tpu as pltpu
from jax.sharding import PartitionSpec as P

NORD = 49152
WIDTH = 128
PANELS = 8
CHIPS = 16
OWN = 32
HALF = CHIPS * OWN
PAIRS = PANELS * (PANELS - 1) // 2
BLOCKS = PAIRS + PANELS // 2
SHARE = BLOCKS * WIDTH // (2 * CHIPS)
PROJ = PANELS * OWN
MORE = PROJ + SHARE
TILE = 16
CHUNK = MORE + TILE
STEP = 256
AHEAD = 5
BF = jnp.bfloat16
F32 = jnp.float32
SIDE = 4


def device(x, z, core):
    return (x * SIDE + z) * 2 + core


def lines(along_z):
    along_x = [[device(x, z, 1 - along_z) for x in range(SIDE)] for z in range(SIDE)]
    return [[device(x, z, along_z) for z in range(SIDE)] for x in range(SIDE)] + along_x


LINES = lines(0)


def swap_pairs(partner):
    return [(line[i], line[partner(i)]) for line in lines(1) for i in range(SIDE)]


SWAPS = (swap_pairs(lambda i: i ^ 1), swap_pairs(lambda i: SIDE - 1 - i))
VMEM = pl.BlockSpec(memory_space=pltpu.VMEM)
HBM = pl.BlockSpec(memory_space=pltpu.HBM)


def call(kernel, out_shape, in_specs, out_specs, flops, nbytes, limit=12, **kw):
    return pl.pallas_call(
        kernel,
        out_shape=out_shape,
        in_specs=in_specs,
        out_specs=out_specs,
        compiler_params=pltpu.CompilerParams(vmem_limit_bytes=limit * 2**20),
        cost_estimate=pl.CostEstimate(flops=flops, bytes_accessed=nbytes, transcendentals=0),
        **kw,
    )


def core_index():
    return lax.rem(lax.axis_index("row"), 2)


def first_block(k):
    return k * (k - 1) // 2


def load(source, target, sem):
    copy = pltpu.make_async_copy(source, target, sem)
    copy.start()
    return copy


def pair(v_ref, k):
    return jnp.concatenate([v_ref[k], v_ref[k + 1]], axis=1)


def parts_of(value):
    parts = []
    for _ in range(3):
        part = value.astype(BF).astype(F32)
        parts.append(part)
        value = value - part
    return parts


def packed(values):
    row = lax.broadcasted_iota(jnp.int32, (TILE, WIDTH), 0)
    tile = jnp.zeros((TILE, WIDTH), F32)
    for i, value in enumerate(values):
        for j, part in enumerate(parts_of(value)):
            tile = jnp.where(row == 3 * i + j, part, tile)
    return tile.astype(BF)


def unpacked(tile, count):
    tile = tile.astype(F32)
    return [
        tile[3 * i : 3 * i + 1] + tile[3 * i + 1 : 3 * i + 2] + tile[3 * i + 2 : 3 * i + 3]
        for i in range(count)
    ]


def squares_of(x):
    wide = x.astype(F32)
    return jnp.sum(wide * wide, axis=0, keepdims=True)


def put(p_ref, n, k, both):
    chips = slice(n // OWN, (n + STEP) // OWN)
    for dk in range(2):
        p_ref[chips, (k + dk) * OWN : (k + dk + 1) * OWN, :] = (
            both[:, dk * WIDTH : (dk + 1) * WIDTH].astype(BF).reshape(STEP // OWN, OWN, WIDTH)
        )


def project(x_ref, v_ref, half, p_ref):
    squares = []
    for n in range(0, HALF, STEP):
        x = x_ref[:, pl.ds(pl.multiple_of(half * HALF + n, STEP), STEP)]
        squares.append(squares_of(x))
        xt = x.T
        for k in range(0, PANELS, 2):
            put(p_ref, n, k, jnp.dot(xt, pair(v_ref, k), preferred_element_type=F32))
    return jnp.concatenate(squares, axis=1)


def group_of(values, s):
    at = s * OWN // WIDTH * WIDTH
    return values[:, at : at + WIDTH]


def first_kernel(
    x_hbm, v_hbm, other_ref, mine_ref, diag_ref, x_ref, v_ref, xt_ref, vt_ref, sems
):
    core = core_index()
    half = 1 - core

    def columns(half, n):
        return pl.ds(pl.multiple_of(half * HALF + n * STEP, STEP), STEP)

    def of_x(half, n):
        at = columns(half, n)
        return x_hbm.at[:, at], x_ref.at[:, at]

    def of_v(k):
        return v_hbm.at[2 * k : 2 * k + 2], v_ref.at[2 * k : 2 * k + 2]

    queue = [of_x(half, 0), of_v(0), of_v(1), of_x(half, 1), of_v(2), of_v(3)]
    queue += [of_x(core, 0), of_x(core, 1)]
    copies = []

    def start():
        if len(copies) < len(queue):
            copies.append(load(*queue[len(copies)], sems.at[len(copies)]))

    def arrived(i):
        copies[i].wait()
        start()

    for _ in range(AHEAD):
        start()
    row = lax.broadcasted_iota(jnp.int32, (WIDTH, WIDTH), 0)
    column = lax.broadcasted_iota(jnp.int32, (WIDTH, WIDTH), 1)
    squares = [None] * (HALF // STEP)
    diag = []

    def turn(n):
        x = x_ref[:, columns(half, n)]
        xt_ref[n] = x.T
        squares[n] = squares_of(x)

    def product(n, k):
        put(
            other_ref,
            n * STEP,
            2 * k,
            jnp.dot(xt_ref[n], pair(v_ref, 2 * k), preferred_element_type=F32),
        )

    def keep(block, value):
        sent = core != block // CHIPS
        value = value.astype(BF)
        spot = block % CHIPS
        other_ref[jnp.where(sent, spot, CHIPS), PROJ:MORE, :] = value
        mine_ref[jnp.where(sent, CHIPS, spot)] = value

    def gram(j, k):
        both = jnp.dot(vt_ref[j], pair(v_ref, 2 * k), preferred_element_type=F32)
        blocks = [
            [both[d * WIDTH : (d + 1) * WIDTH, e * WIDTH : (e + 1) * WIDTH] for e in range(2)]
            for d in range(2)
        ]
        for d in range(2):
            for e in range(2):
                if 2 * j + d < 2 * k + e:
                    keep(first_block(2 * k + e) + 2 * j + d, blocks[d][e])
        if j == k:
            keep(PAIRS + k, jnp.where(row < column, blocks[0][0], blocks[1][1]))
            for d in range(2):
                own = jnp.where(row == column, blocks[d][d], 0.0)
                diag.append(jnp.sum(own, axis=0, keepdims=True))

    def panels(k, tiles):
        vt_ref[k] = pair(v_ref, 2 * k).T
        for n in tiles:
            product(n, k)
        for j in range(k + 1):
            gram(j, k)

    arrived(0)
    turn(0)
    arrived(1)
    panels(0, [0])
    arrived(2)
    panels(1, [0])
    arrived(3)
    turn(1)
    product(1, 0)
    product(1, 1)
    arrived(4)
    panels(2, [0, 1])
    arrived(5)
    panels(3, [0, 1])
    squares = jnp.concatenate(squares, axis=1)
    for k in range(PANELS):
        diag_ref[k : k + 1, :] = diag[k]
    for s in range(CHIPS):
        other_ref[s, MORE:, :] = packed([group_of(squares, s), diag[s % PANELS]])
    arrived(6)
    arrived(7)


def own_kernel(x_ref, v_ref, p_ref, sq_ref):
    sq_ref[...] = project(x_ref, v_ref, core_index(), p_ref)


def combine_kernel(own_ref, sq_ref, gram_ref, diag_ref, other_ref, out_ref):
    for s in range(CHIPS):
        out_ref[s, :PROJ, :] = (
            own_ref[s].astype(F32) + other_ref[s, :PROJ, :].astype(F32)
        ).astype(BF)
        out_ref[s, PROJ:MORE, :] = (
            gram_ref[s].astype(F32) + other_ref[s, PROJ:MORE, :].astype(F32)
        ).astype(BF)
        squares, diag = unpacked(other_ref[s, MORE:, :], 2)
        k = s % PANELS
        out_ref[s, MORE:, :] = packed(
            [group_of(sq_ref[...], s) + squares, diag_ref[k : k + 1, :] + diag]
        )


def sum_tiles(parts, at):
    total = parts[0].astype(F32)
    for part in parts[1:]:
        total = total + part.astype(F32)
    return packed(unpacked(total, 2)) if at == MORE else total.astype(BF)


def sum_kernel(parts_ref, out_ref):
    for i in range(SIDE):
        for at in range(0, CHUNK, TILE):
            here = slice(i * CHUNK + at, i * CHUNK + at + TILE)
            parts = [parts_ref[s, here, :] for s in range(SIDE)]
            out_ref[i, at : at + TILE, :] = sum_tiles(parts, at)


def add_kernel(mine_ref, theirs_ref, out_ref):
    for i in range(SIDE):
        for at in range(0, CHUNK, TILE):
            here = slice(at, at + TILE)
            total = sum_tiles([mine_ref[i, here, :], theirs_ref[i, here, :]], at)
            if out_ref.shape[1] == CHUNK:
                out_ref[i, here, :] = total
            else:
                for j in range(SIDE):
                    out_ref[j, i * CHUNK + at : i * CHUNK + at + TILE, :] = total


def split(value):
    high = value.astype(BF)
    return high, (value - high.astype(F32)).astype(BF)


def solve_kernel(mine_ref, theirs_ref, t_ref, out_ref, dev_ref, g_ref):
    core = core_index()
    for s in range(CHIPS):
        at = pl.multiple_of(core * CHIPS * SHARE + s * SHARE, 16)
        g_ref[pl.ds(at, SHARE), :] = mine_ref[s, PROJ:MORE, :]
        at = pl.multiple_of((1 - core) * CHIPS * SHARE + s * SHARE, 16)
        g_ref[pl.ds(at, SHARE), :] = theirs_ref[s]
    row = lax.broadcasted_iota(jnp.int32, (WIDTH, WIDTH), 0)
    column = lax.broadcasted_iota(jnp.int32, (WIDTH, WIDTH), 1)
    done = []
    change = jnp.zeros((HALF, WIDTH), F32)
    for k in range(PANELS + 1):
        rows = slice(k * OWN, (k + 1) * OWN)
        if k:
            at = (PAIRS + (k - 1) // 2) * WIDTH
            own = g_ref[at : at + WIDTH, :].astype(F32)
            own = jnp.where(row < column if k % 2 else row > column, 2.0 * own, 0.0).astype(BF)
            if k > 1:
                own = jnp.concatenate([jnp.zeros(((k - 1) * WIDTH, WIDTH), BF), own], axis=0)
            right = own
            if k < PANELS:
                at = first_block(k) * WIDTH
                right = jnp.concatenate([g_ref[at : at + k * WIDTH, :], own], axis=1)
            else:
                right, done = own[-WIDTH:], done[-1:]
            before = jnp.concatenate(done, axis=1) if len(done) > 1 else done[0]
            both = jnp.dot(before, right, preferred_element_type=F32)
            change += done[-1].astype(F32) * both[:, -WIDTH:]
        if k == PANELS:
            break
        proj = mine_ref[:, rows, :].reshape(HALF, WIDTH).astype(F32)
        if k:
            proj = proj - both[:, :WIDTH]
        factor, rest = split(t_ref[k])
        high, low = split(proj)
        scaled = lax.dot_general(
            jnp.concatenate([high, low, high], axis=1),
            jnp.concatenate([factor, factor, rest], axis=1),
            (((1,), (1,)), ((), ())),
            preferred_element_type=F32,
        ).astype(BF)
        done.append(scaled)
        out_ref[:, rows, :] = scaled.reshape(CHIPS, OWN, WIDTH)
        wide = scaled.astype(F32)
        change += wide * (wide * unpacked(mine_ref[k, MORE:, :], 2)[1] - 2.0 * proj)
    squares = jnp.sum(change.T, axis=0, keepdims=True)
    before = jnp.concatenate(
        [
            unpacked(mine_ref[s, MORE:, :], 2)[0]
            for s in range(0, CHIPS, WIDTH // OWN)
        ],
        axis=1,
    )
    deviation = jnp.sqrt(jnp.maximum(before + squares, 0.0) / NORD) - 1.0
    dev_ref[...] = deviation
    tile = packed([deviation[:, n : n + WIDTH] for n in range(0, HALF, WIDTH)])
    for s in range(CHIPS):
        out_ref[s, PROJ:, :] = tile


def update_kernel(flip, x_ref, v_ref, s_ref, *refs):
    out_hbm, *more, out_ref, sem = refs[2:] if flip else refs
    core = core_index()
    half = 1 - core if flip else core
    left = jnp.concatenate([v_ref[k] for k in range(PANELS)], axis=1)
    for n in range(0, HALF, STEP):
        chips = slice(n // OWN, (n + STEP) // OWN)
        right = jnp.concatenate(
            [s_ref[chips, k * OWN : (k + 1) * OWN, :].reshape(STEP, WIDTH) for k in range(PANELS)],
            axis=1,
        )
        update = lax.dot_general(left, right, (((1,), (1,)), ((), ())), preferred_element_type=F32)
        columns = pl.ds(pl.multiple_of(half * HALF + n, STEP), STEP)
        out_ref[:, n : n + STEP] = (x_ref[:, columns].astype(F32) - update).astype(BF)
    columns = pl.ds(pl.multiple_of(half * HALF, HALF), HALF)
    store = load(out_ref, out_hbm.at[:, columns], sem)
    if flip:
        theirs = jnp.concatenate(unpacked(s_ref[0, PROJ:, :], HALF // WIDTH), axis=1)
        more[0][:, pl.ds(pl.multiple_of(core * HALF, HALF), HALF)] = refs[1][...]
        more[0][:, pl.ds(pl.multiple_of(half * HALF, HALF), HALF)] = theirs
    store.wait()


def update(flip, eigvecs, reflectors, scaled, *so_far):
    rows = eigvecs.shape[0]
    in_specs = [VMEM] * 3
    out_shape = jax.ShapeDtypeStruct(eigvecs.shape, BF)
    out_specs = HBM
    aliases = {}
    if flip:
        in_specs += [HBM, VMEM]
        aliases = {3: 0}
        out_shape = (out_shape, jax.ShapeDtypeStruct((1, 2 * HALF), F32))
        out_specs = (HBM, VMEM)
    return call(
        functools.partial(update_kernel, flip),
        out_shape,
        in_specs,
        out_specs,
        2 * rows * HALF * PANELS * WIDTH,
        6 * 2**20,
        input_output_aliases=aliases,
        scratch_shapes=[
            pltpu.VMEM((rows, HALF), BF),
            pltpu.SemaphoreType.DMA,
        ],
    )(eigvecs, reflectors, scaled, *so_far)


CORES = [(i ^ 1, i) for i in range(2 * CHIPS)]


def swapped(value, pairs=CORES):
    return lax.ppermute(value, "row", pairs)


def exchanged(value):
    return lax.all_to_all(
        value, "row", split_axis=0, concat_axis=0, axis_index_groups=LINES, tiled=True
    )


def steps(eigvecs, reflectors, factors):
    rows = eigvecs.shape[0]
    flops = 2 * rows * HALF * PANELS * WIDTH
    chunks = jax.ShapeDtypeStruct((CHIPS, CHUNK, WIDTH), BF)
    tiles = HALF // STEP
    other, gram, diag, eigvecs, reflectors = call(
        first_kernel,
        (
            pltpu.VMEM((CHIPS + 1, CHUNK, WIDTH), BF),
            pltpu.VMEM((CHIPS + 1, SHARE, WIDTH), BF),
            pltpu.VMEM((PANELS, WIDTH), F32),
            pltpu.VMEM(eigvecs.shape, BF),
            pltpu.VMEM(reflectors.shape, BF),
        ),
        [HBM] * 2,
        (VMEM,) * 5,
        2 * flops,
        8 * 2**20,
        limit=54,
        scratch_shapes=[
            pltpu.VMEM((tiles, STEP, rows), BF),
            pltpu.VMEM((PANELS // 2, 2 * WIDTH, rows), BF),
            pltpu.SemaphoreType.DMA((2 * tiles + PANELS // 2,)),
        ],
    )(eigvecs, reflectors)
    other = swapped(other)
    own, squares = call(
        own_kernel,
        (
            jax.ShapeDtypeStruct((CHIPS, PROJ, WIDTH), BF),
            jax.ShapeDtypeStruct((1, HALF), F32),
        ),
        [VMEM] * 2,
        (VMEM,) * 2,
        flops,
        6 * 2**20,
    )(eigvecs, reflectors)
    payload = call(combine_kernel, chunks, [VMEM] * 5, VMEM, 2**20, 4 * 2**20)(
        own, squares, gram, diag, other
    )
    lot = jax.ShapeDtypeStruct((SIDE, CHUNK, WIDTH), BF)
    lots = jax.ShapeDtypeStruct((SIDE, SIDE * CHUNK, WIDTH), BF)
    parts = exchanged(payload.reshape(SIDE, -1, WIDTH))
    sums = call(sum_kernel, lot, [VMEM], VMEM, 2**20, 2 * 2**20)(parts)
    for pairs, shape in zip(SWAPS, (lot, lots)):
        theirs = swapped(sums, pairs)
        sums = call(add_kernel, shape, [VMEM] * 2, VMEM, 2**20, 2 * 2**20)(sums, theirs)
    mine = exchanged(sums).reshape(CHIPS, CHUNK, WIDTH)
    theirs = swapped(mine[:, PROJ:MORE, :])
    scaled, dev = call(
        solve_kernel,
        (
            jax.ShapeDtypeStruct((CHIPS, PROJ + TILE, WIDTH), BF),
            jax.ShapeDtypeStruct((1, HALF), F32),
        ),
        [VMEM] * 3,
        (VMEM,) * 2,
        2**28,
        4 * 2**20,
        scratch_shapes=[pltpu.VMEM((BLOCKS * WIDTH, WIDTH), BF)],
    )(mine, theirs, factors)
    scaled_theirs = swapped(scaled)
    vectors = update(False, eigvecs, reflectors, scaled)
    vectors, deviation = update(True, eigvecs, reflectors, scaled_theirs, vectors, dev)
    return (vectors, deviation.reshape(-1))


def solution(mesh):
    placed = (P("row", "col"), P(None, "row", None), P())
    return jax.shard_map(
        steps, mesh=mesh, in_specs=placed, out_specs=(P("row", "col"), P("col")), check_vma=False
    )
```
